32 devices in a mesh: group: 8 (over z, x), rad: 4 (over y, core).
Axes of the slice: x: 2, y: 2, z: 4, core: 2. Of those that a mesh axis runs over, the one named last changes fastest.
Arguments:
- source_term: float32 [32, 128, 1024], P('group', 'rad'), may hold values from -6 to 6
- initial_guess: float32 [32, 128, 1024], P('group', 'rad'), may hold values from -3 to 3
- metric: float32 [3, 8, 32, 256], P(None, 'group', 'rad'), may hold values from 0.5 to 4
Outputs:
- solution: float32 [32, 128, 1024], P('group', 'rad')
- residual: float32 [32, 128, 1024], P('group', 'rad')
The draws below stay inside these ranges and needn't reach their ends.
All inputs are finite; a program needn't handle non-finite values.
Results may differ from the reference program's by a relative error of at most 0.00025.
Values sent between devices are 32-bit elements; how exact they have to be, the bound alone decides.
A program may use at most 128 MiB of HBM per device.

```python
import math
import jax
import jax.numpy as jnp
import numpy as np
from jax import lax

EY = 256
ITERS = 3
NEX = 8
NER = 32
NX = 32
NR = 128
NY = 1024


def block_levels(key, extent, shards, least, high):
    def one(position, blocks):
        steps = jax.random.uniform(jax.random.fold_in(jax.random.fold_in(key, 6), position), (blocks,), jnp.float32, least / len(shards), high / len(shards))
        return jnp.repeat(jnp.exp(steps), extent[position] // blocks).reshape((-1,) + (1,) * (len(extent) - position - 1))

    level = one(*shards[0])
    for cut in shards[1:]:
        level = level * one(*cut)
    return level


def gaussian(key, shape, width, reach, pieces=(), held_as=jnp.bfloat16):
    values = width * jax.random.normal(key, shape, jnp.float32)
    if pieces:
        values = values * block_levels(key, shape, pieces, -0.22, 0.18)
    return jnp.clip(values, -reach, reach).astype(held_as)


def setup_inputs(seed: int = 0) -> dict:
    streams_of = jax.random.split(jax.random.key(seed), 4)
    source_term = gaussian(streams_of[0], (NX, NR, NY), 1.0, 6.0, ((0, 8), (1, 4)), jnp.float32)
    initial_guess = gaussian(streams_of[1], (NX, NR, NY), 0.5, 3.0, ((0, 8), (1, 4)), jnp.float32)
    metric = jnp.clip(jnp.exp(math.log(4.0) - 2.0794415 * jax.random.uniform(streams_of[2], (3, NEX, NER, EY), jnp.float32) ** block_levels(streams_of[2], (3, NEX, NER, EY), ((1, 8), (2, 4)), -0.2, 0.2)), 0.5, 4.0)
    return dict(source_term=source_term, initial_guess=initial_guess, metric=metric)


def gll_tables():
    root = math.sqrt(3.0 / 7.0)
    points = np.array([-1.0, -root, 0.0, root, 1.0])
    weights = np.array([0.1, 49.0 / 90.0, 32.0 / 45.0, 49.0 / 90.0, 0.1])
    factor = np.array([np.prod([points[a] - points[m] for m in range(5) if m != a]) for a in range(5)])
    derivative = np.zeros((5, 5))
    for p in range(5):
        for a in range(5):
            if p == a:
                derivative[p, a] = np.sum([1.0 / (points[a] - points[m]) for m in range(5) if m != a])
            else:
                derivative[p, a] = factor[p] / (factor[a] * (points[p] - points[a]))
    return (jnp.asarray(derivative, jnp.float32), jnp.asarray(weights, jnp.float32))

def take_every(values, first, number, dim_axis):
    return lax.slice_in_dim(values, first, first + 4 * (number - 1) + 1, 4, dim_axis)

def to_elements(extended, count_x, count_r, count_y):
    layers = [take_every(extended, k, count_y, 2) for k in range(4)]
    layers.append(jnp.roll(layers[0], -1, axis=2))
    stacked = jnp.stack(layers, 0)
    across = jnp.stack([take_every(stacked, i, count_x, 1) for i in range(5)], 0)
    return jnp.stack([take_every(across, j, count_r, 3) for j in range(5)], 1)

def spread(values, low_pad, high_pad, dim_axis):
    config = [(0, 0, 0)] * values.ndim
    config[dim_axis] = (low_pad, high_pad, 3)
    return lax.pad(values, jnp.zeros((), values.dtype), config)

def from_elements(result):
    along_r = spread(result[:, 0], 0, 4, 3)
    for j in range(1, 5):
        along_r = along_r + spread(result[:, j], j, 4 - j, 3)
    along_x = spread(along_r[0], 0, 4, 1)
    for i in range(1, 5):
        along_x = along_x + spread(along_r[i], i, 4 - i, 1)
    first = along_x[0] + jnp.roll(along_x[4], 1, axis=2)
    total = spread(first, 0, 3, 2)
    for k in range(1, 4):
        total = total + spread(along_x[k], k, 3 - k, 2)
    return total

def apply_elements(elements, metric):
    derivative, weights = gll_tables()
    derivative = derivative.astype(elements.dtype)
    weights = weights.astype(elements.dtype)
    quad_weight = (weights[:, None, None] * weights[None, :, None] * weights[None, None, :]).reshape(5, 5, 5, 1, 1, 1)
    high = lax.Precision.HIGHEST
    grad_x = jnp.einsum('pa,abcxyz->pbcxyz', derivative, elements, precision=high)
    result_sum = jnp.einsum('pa,pbcxyz->abcxyz', derivative, grad_x * quad_weight * metric[0], precision=high)
    grad_r = jnp.einsum('qb,abcxyz->aqcxyz', derivative, elements, precision=high)
    result_sum = result_sum + jnp.einsum('qb,aqcxyz->abcxyz', derivative, grad_r * quad_weight * metric[1], precision=high)
    grad_y = jnp.einsum('sc,abcxyz->absxyz', derivative, elements, precision=high)
    result_sum = result_sum + jnp.einsum('sc,absxyz->abcxyz', derivative, grad_y * quad_weight * metric[2], precision=high)
    return result_sum

def element_diagonal(metric):
    derivative, weights = gll_tables()
    derivative = derivative.astype(metric.dtype)
    weights = weights.astype(metric.dtype)
    squared = lax.optimization_barrier(jnp.sum(derivative * derivative * weights[:, None], axis=0))
    term_x = (squared[:, None, None] * weights[None, :, None] * weights[None, None, :]).reshape(5, 5, 5, 1, 1, 1)
    term_r = (weights[:, None, None] * squared[None, :, None] * weights[None, None, :]).reshape(5, 5, 5, 1, 1, 1)
    term_y = (weights[:, None, None] * weights[None, :, None] * squared[None, None, :]).reshape(5, 5, 5, 1, 1, 1)
    return term_x * metric[0] + term_r * metric[1] + term_y * metric[2]

def fold_cycle(raw):
    last_x = raw.shape[0] - 1
    last_r = raw.shape[1] - 1
    interior = raw[:last_x, :last_r]
    return jnp.concatenate([interior[0:1] + raw[last_x:, :last_r], interior[1:]], 0)

def operate(field, metric):
    extended = jnp.concatenate([field, field[0:1]], 0)
    extended = jnp.concatenate([extended, jnp.zeros_like(extended[:, 0:1])], 1)
    elements = to_elements(extended, metric.shape[1], metric.shape[2], metric.shape[3])
    return fold_cycle(from_elements(apply_elements(elements, metric)))

def reference(source_term, initial_guess, metric):
    diagonal = fold_cycle(from_elements(element_diagonal(metric)))
    scaling = 1.0 / diagonal
    residual = source_term - operate(initial_guess, metric)
    solution = initial_guess
    smoothed = scaling * residual
    direction = smoothed
    weighted_norm = jnp.sum(residual * smoothed)
    for iteration in range(ITERS):
        applied = operate(direction, metric)
        step_size = weighted_norm / jnp.sum(direction * applied)
        solution = solution + step_size * direction
        residual = residual - step_size * applied
        if iteration + 1 < ITERS:
            smoothed = scaling * residual
            next_norm = jnp.sum(residual * smoothed)
            direction = smoothed + next_norm / weighted_norm * direction
            weighted_norm = next_norm
    return (solution, residual)
```

```python
import functools
import math

import jax
import jax.numpy as jnp
import numpy as np
from jax import lax
from jax.experimental import pallas as pl
from jax.experimental.pallas import tpu as pltpu
from jax.sharding import PartitionSpec as P

MESH = pl.DeviceIdType.MESH
ITERS = 3
APPLIES = ITERS + 1
CHUNK = 512
F32 = jnp.float32
BF16 = jnp.bfloat16


def gll_tables():
    root = math.sqrt(3.0 / 7.0)
    points = np.array([-1.0, -root, 0.0, root, 1.0])
    weights = np.array([0.1, 49.0 / 90.0, 32.0 / 45.0, 49.0 / 90.0, 0.1])
    factor = np.array(
        [np.prod([points[a] - points[m] for m in range(5) if m != a]) for a in range(5)]
    )
    derivative = np.zeros((5, 5))
    for p in range(5):
        for a in range(5):
            if p == a:
                derivative[p, a] = np.sum(
                    [1.0 / (points[a] - points[m]) for m in range(5) if m != a]
                )
            else:
                derivative[p, a] = factor[p] / (factor[a] * (points[p] - points[a]))
    return derivative, weights


DERIVATIVE, WEIGHTS = gll_tables()
STIFF = [[float(v) for v in row] for row in DERIVATIVE.T @ (WEIGHTS[:, None] * DERIVATIVE)]
W = [float(v) for v in WEIGHTS]


def combine(row, tiles):
    total = tiles[0] * STIFF[row][0]
    for other in range(1, 4):
        total = total + tiles[other] * STIFF[row][other]
    return total


def exact_pieces(value):
    high = value.astype(BF16)
    rest = value - high.astype(F32)
    middle = rest.astype(BF16)
    low = (rest - middle.astype(F32)).astype(BF16)
    return high, middle, low


def dot(left, right):
    return jnp.dot(left, right, preferred_element_type=F32)


def one_where(condition):
    return jnp.where(condition, 1.0, 0.0).astype(BF16)


def kernel(
    n_group, n_rad, source_hbm, guess_hbm, metric_hbm, sol_hbm, res_hbm,
    source_in, guess_in, own, prev, below, diag,
    c0, c0p, c1, c1s, c2, c2s, inv,
    x, r, u, w, m_first, m_second, n, z, s, p,
    plane_out, plane_in, part_in, row_out, row_in, rowpart_out, rowpart_in,
    rad_out, rad_in, group_out, group_in,
    local_sem, met_send, met_recv, halo_send, halo_recv,
    rad_send, rad_recv, group_send, group_recv,
):
    e = lax.axis_index("group")
    k = lax.axis_index("rad")
    nxt, prv = lax.rem(e + 1, n_group), lax.rem(e + n_group - 1, n_group)
    up, down = lax.rem(k + 1, n_rad), lax.rem(k + n_rad - 1, n_rad)
    has_below = jnp.where(k == 0, 0.0, 1.0).astype(F32)
    has_above = jnp.where(k == n_rad - 1, 0.0, 1.0).astype(F32)
    rows, width = own.shape[1:]
    nodes, lanes = 16 * rows, 4 * width
    last = rows - 1

    loads = [
        pltpu.make_async_copy(metric_hbm, own, local_sem.at[0]),
        pltpu.make_async_copy(guess_hbm, guess_in, local_sem.at[1]),
        pltpu.make_async_copy(source_hbm, source_in, local_sem.at[2]),
    ]
    for load in loads:
        load.start()

    barrier = pltpu.get_barrier_semaphore()
    for d in range(1, n_group):
        pl.semaphore_signal(
            barrier, inc=1, device_id=(lax.rem(e + d, n_group), k), device_id_type=MESH
        )
    for d in range(1, n_rad):
        pl.semaphore_signal(
            barrier, inc=1, device_id=(e, lax.rem(k + d, n_rad)), device_id_type=MESH
        )
    pl.semaphore_signal(barrier, inc=1, device_id=(nxt, up), device_id_type=MESH)
    pl.semaphore_signal(barrier, inc=1, device_id=(prv, down), device_id_type=MESH)

    i0 = lax.broadcasted_iota(jnp.int32, (CHUNK, CHUNK), 0)
    i1 = lax.broadcasted_iota(jnp.int32, (CHUNK, CHUNK), 1)
    part = CHUNK // 4
    lane_split = one_where(i0 == 4 * (i1 % part) + i1 // part)
    r0 = lax.broadcasted_iota(jnp.int32, (nodes, nodes), 0)
    r1 = lax.broadcasted_iota(jnp.int32, (nodes, nodes), 1)
    block = 4 * rows

    def split_row(i):
        return (i // block) * block + 4 * (i % rows) + (i % block) // rows

    row_split = one_where(r1 == split_row(r0))

    def to_blocks(field_in, target):
        pieces = exact_pieces(field_in[...].reshape(nodes, lanes))
        pieces = [dot(row_split, piece).astype(BF16) for piece in pieces]
        for h in range(lanes // CHUNK):
            cut = slice(h * CHUNK, (h + 1) * CHUNK)
            moved = dot(pieces[0][:, cut], lane_split)
            moved = moved + dot(pieces[1][:, cut], lane_split)
            moved = moved + dot(pieces[2][:, cut], lane_split)
            moved = moved.reshape(4, 4, rows, CHUNK)
            for c in range(4):
                target[:, :, c, :, h * part:(h + 1) * part] = (
                    moved[:, :, :, c * part:(c + 1) * part]
                )

    pl.semaphore_wait(barrier, n_group + n_rad)

    def remote(src, dst, send, recv, where):
        return pltpu.make_async_remote_copy(
            src_ref=src, dst_ref=dst, send_sem=send, recv_sem=recv,
            device_id=where, device_id_type=MESH,
        )

    loads[0].wait()
    metric_moves = [
        remote(own, prev, met_send.at[0], met_recv.at[0], (nxt, k)),
        remote(own, below, met_send.at[1], met_recv.at[1], (e, up)),
        remote(own, diag, met_send.at[2], met_recv.at[2], (nxt, up)),
    ]
    for move in metric_moves:
        move.start()

    loads[1].wait()
    to_blocks(guess_in, x)

    row_index = lax.broadcasted_iota(jnp.int32, (rows, width), 0)
    first_row, last_row = row_index == 0, row_index == last

    def shift_y(tile):
        return pltpu.roll(tile, 1, 1)

    def next_y(tile):
        return pltpu.roll(tile, width - 1, 1)

    def moves_of(j, v):
        return [
            remote(v.at[0], plane_in.at[j], halo_send.at[j, 0], halo_recv.at[j, 0], (prv, k)),
            remote(row_out.at[j], row_in.at[j], halo_send.at[j, 1], halo_recv.at[j, 1], (e, down)),
            remote(rowpart_out.at[j], rowpart_in.at[j], halo_send.at[j, 2], halo_recv.at[j, 2], (e, up)),
            remote(plane_out.at[j], part_in.at[j], halo_send.at[j, 3], halo_recv.at[j, 3], (nxt, k)),
        ]

    def looped(body):
        def step(i, carry):
            body(i)
            return carry

        lax.fori_loop(0, 4, step, 0)

    def start_plane(j, v):
        moves_of(j, v)[0].start()

    def start_rest(j, v):
        moves = moves_of(j, v)

        def plane(b):
            for c in range(4):
                plane_out[j, b, c] = c0[b, c] * combine(4, [v[a, b, c] for a in range(4)])

        looped(plane)
        moves[3].start()

        def edge(a):
            for c in range(4):
                row_out[j, a, pl.ds(c, 1), :] = v[a, 0, c, pl.ds(0, 1), :]
                rowpart_out[j, a, pl.ds(c, 1), :] = c1[a, c, pl.ds(last, 1), :] * combine(
                    4, [v[a, b, c, pl.ds(last, 1), :] for b in range(4)]
                )

        looped(edge)
        moves[1].start()
        moves[2].start()

    def local_part(v, out):
        def along_x(b):
            for c in range(4):
                tiles = [v[a, b, c] for a in range(4)]
                scale = c0[b, c]
                out[0, b, c] = scale * combine(0, tiles) + c0p[b, c] * tiles[0]
                for a in range(1, 4):
                    out[a, b, c] = scale * combine(a, tiles)

        looped(along_x)

        def along_r(a):
            for c in range(4):
                tiles = [v[a, b, c] for b in range(4)]
                scale = c1[a, c]
                above = jnp.where(last_row, 0.0, pltpu.roll(tiles[0], rows - 1, 0))
                carried = jnp.where(first_row, 0.0, pltpu.roll(scale * combine(4, tiles), 1, 0))
                for b in range(4):
                    value = scale * (combine(b, tiles) + above * STIFF[b][4])
                    if b == 0:
                        value = value + carried + c1s[a, c] * tiles[0]
                    out[a, b, c] += value

        looped(along_r)

        def along_y(a):
            for b in range(4):
                tiles = [v[a, b, c] for c in range(4)]
                scale = c2[a, b]
                above = next_y(tiles[0])
                carried = shift_y(scale * combine(4, tiles))
                for c in range(4):
                    value = scale * (combine(c, tiles) + above * STIFF[c][4])
                    if c == 0:
                        value = value + carried + c2s[a, b] * tiles[0]
                    out[a, b, c] += value

        looped(along_y)

    def finish(j, v, out):
        moves = moves_of(j, v)
        moves[1].wait()
        moves[2].wait()

        def edge(a):
            for c in range(4):
                above = (has_above * row_in[j, a, pl.ds(c, 1), :]) * c1[a, c, pl.ds(last, 1), :]
                for b in range(4):
                    out[a, b, c, pl.ds(last, 1), :] += above * STIFF[b][4]
                out[a, 0, c, pl.ds(0, 1), :] += has_below * rowpart_in[j, a, pl.ds(c, 1), :]

        looped(edge)
        moves[0].wait()
        moves[3].wait()

        def plane(b):
            for c in range(4):
                above = c0[b, c] * plane_in[j, b, c]
                out[0, b, c] += above * STIFF[0][4] + part_in[j, b, c]
                for a in range(1, 4):
                    out[a, b, c] += above * STIFF[a][4]

        looped(plane)

    start_plane(0, x)
    for move in metric_moves:
        move.wait()

    def lower(tile, tile_below):
        edge_row = has_below * tile_below[last:, :]
        return jnp.where(first_row, edge_row, pltpu.roll(tile, 1, 0))

    def four(plain, other, along):
        both = plain + other
        return {
            (0, 0): plain, (1, 0): both,
            (0, 1): plain + along(plain), (1, 1): both + along(both),
        }

    def pick(table, first, second):
        scale = W[first] * W[second]
        return table[(int(first == 0), int(second == 0))] * scale

    own_0, own_1, own_2 = own[0], own[1], own[2]
    prev_0, prev_1, prev_2 = prev[0], prev[1], prev[2]
    below_0, below_1, below_2 = below[0], below[1], below[2]
    diag_0, diag_1, diag_2 = diag[0], diag[1], diag[2]
    table_0 = four(own_0, lower(own_0, below_0), shift_y)
    table_0p = four(prev_0, lower(prev_0, diag_0), shift_y)
    table_1 = four(own_1, prev_1, shift_y)
    table_1b = four(below_1, diag_1, shift_y)
    lower_2, lower_2p = lower(own_2, below_2), lower(prev_2, diag_2)
    table_2 = {
        (0, 0): own_2, (0, 1): own_2 + lower_2,
        (1, 0): own_2 + prev_2, (1, 1): own_2 + lower_2 + prev_2 + lower_2p,
    }
    for i in range(4):
        for j in range(4):
            c0[i, j] = pick(table_0, i, j)
            c0p[i, j] = pick(table_0p, i, j) * STIFF[4][4]
            line = pick(table_1, i, j)
            c1[i, j] = line
            c1s[i, j] = lower(line, pick(table_1b, i, j)) * STIFF[4][4]
            line = pick(table_2, i, j)
            c2[i, j] = line
            c2s[i, j] = shift_y(line) * STIFF[4][4]

    start_rest(0, x)
    loads[2].wait()
    to_blocks(source_in, r)

    def diagonal(a):
        for b in range(4):
            for c in range(4):
                zero_a = jnp.where(a == 0, 1.0, 0.0).astype(F32)
                middle = jnp.where(a == 2, STIFF[2][2], STIFF[1][1]).astype(F32)
                stiff = jnp.where(a == 0, STIFF[0][0], middle).astype(F32)
                total = c0[b, c] * stiff + c0p[b, c] * zero_a
                total = total + c1[a, c] * STIFF[b][b]
                total = total + c2[a, b] * STIFF[c][c]
                if b == 0:
                    total = total + c1s[a, c]
                if c == 0:
                    total = total + c2s[a, b]
                inv[a, b, c] = 1.0 / total

    looped(diagonal)
    local_part(x, n)
    finish(0, x, n)

    def initial(a):
        for b in range(4):
            for c in range(4):
                residual = r[a, b, c] - n[a, b, c]
                r[a, b, c] = residual
                u[a, b, c] = inv[a, b, c] * residual

    looped(initial)

    start_plane(1, u)
    start_rest(1, u)
    local_part(u, w)
    finish(1, u, w)

    def rad_moves(t):
        return [
            remote(rad_out.at[t], rad_in.at[t, d - 1], rad_send.at[t, d - 1],
                   rad_recv.at[t, d - 1], (e, lax.rem(k + d, n_rad)))
            for d in range(1, n_rad)
        ]

    def group_moves(t):
        return [
            remote(group_out.at[t], group_in.at[t, d - 1], group_send.at[t, d - 1],
                   group_recv.at[t, d - 1], (lax.rem(e + d, n_group), k))
            for d in range(1, n_group)
        ]

    def lane_sum(tile):
        row = jnp.sum(tile, axis=0, keepdims=True)
        total = row[:, :128]
        for h in range(1, width // 128):
            total = total + row[:, h * 128:(h + 1) * 128]
        return total

    def sums_begin(t, gamma_tile, delta_tile):
        index = lax.broadcasted_iota(jnp.int32, (8, 128), 0)
        rad_out[t] = jnp.where(
            index == 0, lane_sum(gamma_tile), jnp.where(index == 1, lane_sum(delta_tile), 0.0)
        )
        for move in rad_moves(t):
            move.start()

    def sums_middle(t):
        total = rad_out[t]
        for d, move in enumerate(rad_moves(t)):
            move.wait()
            total = total + rad_in[t, d]
        group_out[t] = total
        for move in group_moves(t):
            move.start()

    def sums_end(t):
        total = group_out[t]
        for d, move in enumerate(group_moves(t)):
            move.wait()
            total = total + group_in[t, d]
        total = jnp.sum(total, axis=1, keepdims=True)
        return total[0:1, :], total[1:2, :]

    def carried_loop(body):
        zero = jnp.zeros((rows, width), F32)
        return lax.fori_loop(0, 4, body, (zero, zero))

    def first_sums(a, carry):
        gamma, delta = carry
        for b in range(4):
            for c in range(4):
                value, applied = u[a, b, c], w[a, b, c]
                gamma = gamma + r[a, b, c] * value
                delta = delta + applied * value
                m_first[a, b, c] = inv[a, b, c] * applied
        return gamma, delta

    tiles = carried_loop(first_sums)
    sums_begin(0, *tiles)
    start_plane(2, m_first)
    start_rest(2, m_first)
    sums_middle(0)
    local_part(m_first, z)
    finish(2, m_first, z)
    gamma_0, delta_0 = sums_end(0)
    alpha_0 = gamma_0 / delta_0
    step = jnp.broadcast_to(alpha_0, (rows, width))

    def first_update(a, carry):
        gamma, delta = carry
        for b in range(4):
            for c in range(4):
                applied, search = w[a, b, c], u[a, b, c]
                s[a, b, c] = applied
                p[a, b, c] = search
                x[a, b, c] += step * search
                residual = r[a, b, c] - step * applied
                r[a, b, c] = residual
                scale = inv[a, b, c]
                smooth = scale * residual
                u[a, b, c] = smooth
                applied = applied - step * z[a, b, c]
                w[a, b, c] = applied
                m_second[a, b, c] = scale * applied
                gamma = gamma + residual * smooth
                delta = delta + applied * smooth
        return gamma, delta

    tiles = carried_loop(first_update)
    sums_begin(1, *tiles)
    start_plane(3, m_second)
    start_rest(3, m_second)
    sums_middle(1)
    local_part(m_second, n)
    finish(3, m_second, n)
    gamma_1, delta_1 = sums_end(1)
    beta_0 = gamma_1 / gamma_0
    alpha_1 = gamma_1 / (delta_1 - beta_0 * gamma_1 / alpha_0)
    step_1 = jnp.broadcast_to(alpha_1, (rows, width))
    ratio_1 = jnp.broadcast_to(beta_0, (rows, width))

    def second_update(a, carry):
        gamma, delta = carry
        for b in range(4):
            for c in range(4):
                applied = w[a, b, c]
                searched = applied + ratio_1 * s[a, b, c]
                s[a, b, c] = searched
                search = u[a, b, c] + ratio_1 * p[a, b, c]
                p[a, b, c] = search
                x[a, b, c] += step_1 * search
                residual = r[a, b, c] - step_1 * searched
                r[a, b, c] = residual
                smooth = inv[a, b, c] * residual
                u[a, b, c] = smooth
                applied = applied - step_1 * (n[a, b, c] + ratio_1 * z[a, b, c])
                w[a, b, c] = applied
                gamma = gamma + residual * smooth
                delta = delta + applied * smooth
        return gamma, delta

    tiles = carried_loop(second_update)
    sums_begin(2, *tiles)
    sums_middle(2)
    lane_join = one_where(i1 == 4 * (i0 % part) + i0 // part)
    row_join = one_where(r0 == split_row(r1))
    gamma_2, delta_2 = sums_end(2)
    beta_1 = gamma_2 / gamma_1
    alpha_2 = gamma_2 / (delta_2 - beta_1 * gamma_2 / alpha_1)
    step_2 = jnp.broadcast_to(alpha_2, (rows, width))
    ratio_2 = jnp.broadcast_to(beta_1, (rows, width))

    def last_update(a):
        for b in range(4):
            for c in range(4):
                x[a, b, c] += step_2 * (u[a, b, c] + ratio_2 * p[a, b, c])
                r[a, b, c] -= step_2 * (w[a, b, c] + ratio_2 * s[a, b, c])

    looped(last_update)

    def from_blocks(field, target):
        for h in range(lanes // CHUNK):
            wide = jnp.concatenate(
                [field[:, :, c, :, h * part:(h + 1) * part] for c in range(4)], axis=-1
            ).reshape(nodes, CHUNK)
            total = None
            for piece in exact_pieces(wide):
                moved = dot(piece, lane_join).astype(BF16)
                moved = dot(row_join, moved)
                total = moved if total is None else total + moved
            target[:, :, h * CHUNK:(h + 1) * CHUNK] = total.reshape(4, block, CHUNK)

    from_blocks(x, guess_in)
    store_x = pltpu.make_async_copy(guess_in, sol_hbm, local_sem.at[3])
    store_x.start()
    from_blocks(r, source_in)
    store_r = pltpu.make_async_copy(source_in, res_hbm, local_sem.at[4])
    store_r.start()
    store_x.wait()
    store_r.wait()


def solution(mesh):
    n_group, n_rad = mesh.shape["group"], mesh.shape["rad"]

    def local(source_term, initial_guess, metric):
        shape = source_term.shape
        metric = metric.reshape(3, metric.shape[2], metric.shape[3])
        rows, width = metric.shape[1:]
        assert shape == (4, 4 * rows, 4 * width) and rows % 8 == 0 and shape[2] % CHUNK == 0
        tile = (rows, width)
        field = pltpu.VMEM((4, 4, 4) + tile, F32)
        plane = pltpu.VMEM((4, 4) + tile, F32)
        planes = pltpu.VMEM((APPLIES, 4, 4) + tile, F32)
        edges = pltpu.VMEM((APPLIES, 4, 4, width), F32)
        any_space = pl.BlockSpec(memory_space=pl.ANY)
        return pl.pallas_call(
            functools.partial(kernel, n_group, n_rad),
            out_shape=[jax.ShapeDtypeStruct(shape, F32)] * 2,
            in_specs=[any_space] * 3,
            out_specs=[any_space] * 2,
            scratch_shapes=[
                pltpu.VMEM(shape, F32), pltpu.VMEM(shape, F32),
                *[pltpu.VMEM((3,) + tile, F32)] * 4,
                *[plane] * 6, field,
                *[field] * 10,
                planes, planes, planes, edges, edges, edges, edges,
                pltpu.VMEM((ITERS, 8, 128), F32), pltpu.VMEM((ITERS, n_rad - 1, 8, 128), F32),
                pltpu.VMEM((ITERS, 8, 128), F32), pltpu.VMEM((ITERS, n_group - 1, 8, 128), F32),
                pltpu.SemaphoreType.DMA((5,)),
                pltpu.SemaphoreType.DMA((3,)), pltpu.SemaphoreType.DMA((3,)),
                pltpu.SemaphoreType.DMA((APPLIES, 4)), pltpu.SemaphoreType.DMA((APPLIES, 4)),
                pltpu.SemaphoreType.DMA((ITERS, n_rad - 1)), pltpu.SemaphoreType.DMA((ITERS, n_rad - 1)),
                pltpu.SemaphoreType.DMA((ITERS, n_group - 1)), pltpu.SemaphoreType.DMA((ITERS, n_group - 1)),
            ],
            compiler_params=pltpu.CompilerParams(
                collective_id=0, has_side_effects=True, vmem_limit_bytes=40 * 1024 * 1024
            ),
            name="pcg",
        )(source_term, initial_guess, metric)

    in_specs = (P("group", "rad", None), P("group", "rad", None), P(None, "group", "rad", None))
    out_specs = (P("group", "rad", None), P("group", "rad", None))
    return jax.shard_map(local, mesh=mesh, in_specs=in_specs, out_specs=out_specs, check_vma=False)
```

```python
import functools
import math

import jax
import jax.numpy as jnp
import numpy as np
from jax import lax
from jax.experimental import pallas as pl
from jax.experimental.pallas import tpu as pltpu
from jax.sharding import PartitionSpec as P

MESH = pl.DeviceIdType.MESH
ITERS = 3
APPLIES = ITERS + 1
CHUNK = 512
F32 = jnp.float32
BF16 = jnp.bfloat16


def gll_tables():
    root = math.sqrt(3.0 / 7.0)
    points = np.array([-1.0, -root, 0.0, root, 1.0])
    weights = np.array([0.1, 49.0 / 90.0, 32.0 / 45.0, 49.0 / 90.0, 0.1])
    factor = np.array(
        [np.prod([points[a] - points[m] for m in range(5) if m != a]) for a in range(5)]
    )
    derivative = np.zeros((5, 5))
    for p in range(5):
        for a in range(5):
            if p == a:
                derivative[p, a] = np.sum(
                    [1.0 / (points[a] - points[m]) for m in range(5) if m != a]
                )
            else:
                derivative[p, a] = factor[p] / (factor[a] * (points[p] - points[a]))
    return derivative, weights


DERIVATIVE, WEIGHTS = gll_tables()
STIFF = [[float(v) for v in row] for row in DERIVATIVE.T @ (WEIGHTS[:, None] * DERIVATIVE)]
W = [float(v) for v in WEIGHTS]


def combine(row, tiles):
    total = tiles[0] * STIFF[row][0]
    for other in range(1, 4):
        total = total + tiles[other] * STIFF[row][other]
    return total


def exact_pieces(value):
    high = value.astype(BF16)
    rest = value - high.astype(F32)
    middle = rest.astype(BF16)
    low = (rest - middle.astype(F32)).astype(BF16)
    return high, middle, low


def dot(left, right):
    return jnp.dot(left, right, preferred_element_type=F32)


def one_where(condition):
    return jnp.where(condition, 1.0, 0.0).astype(BF16)


def kernel(
    n_group, n_rad, source_hbm, guess_hbm, metric_hbm, sol_hbm, res_hbm,
    source_in, guess_in, own, prev, below, diag,
    c0, c0p, c1, c1s, c2, c2s, inv,
    x, r, u, w, m_first, m_second, n, z, s, p,
    plane_out, plane_in, part_in, row_out, row_in, rowpart_out, rowpart_in,
    rad_out, rad_in, group_out, group_in,
    local_sem, met_send, met_recv, halo_send, halo_recv, row_send, row_recv,
    rad_send, rad_recv, group_send, group_recv,
):
    e = lax.axis_index("group")
    k = lax.axis_index("rad")
    nxt, prv = lax.rem(e + 1, n_group), lax.rem(e + n_group - 1, n_group)
    up, down = lax.rem(k + 1, n_rad), lax.rem(k + n_rad - 1, n_rad)
    has_below = jnp.where(k == 0, 0.0, 1.0).astype(F32)
    has_above = jnp.where(k == n_rad - 1, 0.0, 1.0).astype(F32)
    rows, width = own.shape[1:]
    nodes, lanes = 16 * rows, 4 * width
    last = rows - 1

    loads = [
        pltpu.make_async_copy(metric_hbm, own, local_sem.at[0]),
        pltpu.make_async_copy(guess_hbm, guess_in, local_sem.at[1]),
        pltpu.make_async_copy(source_hbm, source_in, local_sem.at[2]),
    ]
    for load in loads:
        load.start()

    barrier = pltpu.get_barrier_semaphore()
    for d in range(1, n_group):
        pl.semaphore_signal(
            barrier, inc=1, device_id=(lax.rem(e + d, n_group), k), device_id_type=MESH
        )
    for d in range(1, n_rad):
        pl.semaphore_signal(
            barrier, inc=1, device_id=(e, lax.rem(k + d, n_rad)), device_id_type=MESH
        )
    pl.semaphore_signal(barrier, inc=1, device_id=(nxt, up), device_id_type=MESH)
    pl.semaphore_signal(barrier, inc=1, device_id=(prv, down), device_id_type=MESH)

    i0 = lax.broadcasted_iota(jnp.int32, (CHUNK, CHUNK), 0)
    i1 = lax.broadcasted_iota(jnp.int32, (CHUNK, CHUNK), 1)
    part = CHUNK // 4
    lane_split = one_where(i0 == 4 * (i1 % part) + i1 // part)
    r0 = lax.broadcasted_iota(jnp.int32, (nodes, nodes), 0)
    r1 = lax.broadcasted_iota(jnp.int32, (nodes, nodes), 1)
    block = 4 * rows

    def split_row(i):
        return (i // block) * block + 4 * (i % rows) + (i % block) // rows

    row_split = one_where(r1 == split_row(r0))

    def to_blocks(field_in, target):
        pieces = exact_pieces(field_in[...].reshape(nodes, lanes))
        pieces = [dot(row_split, piece).astype(BF16) for piece in pieces]
        for h in range(lanes // CHUNK):
            cut = slice(h * CHUNK, (h + 1) * CHUNK)
            moved = dot(pieces[0][:, cut], lane_split)
            moved = moved + dot(pieces[1][:, cut], lane_split)
            moved = moved + dot(pieces[2][:, cut], lane_split)
            moved = moved.reshape(4, 4, rows, CHUNK)
            for c in range(4):
                target[:, :, c, :, h * part:(h + 1) * part] = (
                    moved[:, :, :, c * part:(c + 1) * part]
                )

    pl.semaphore_wait(barrier, n_group + n_rad)

    def remote(src, dst, send, recv, where):
        return pltpu.make_async_remote_copy(
            src_ref=src, dst_ref=dst, send_sem=send, recv_sem=recv,
            device_id=where, device_id_type=MESH,
        )

    loads[0].wait()
    metric_moves = [
        remote(own, prev, met_send.at[0], met_recv.at[0], (nxt, k)),
        remote(own, below, met_send.at[1], met_recv.at[1], (e, up)),
        remote(own, diag, met_send.at[2], met_recv.at[2], (nxt, up)),
    ]
    for move in metric_moves:
        move.start()

    loads[1].wait()
    to_blocks(guess_in, x)

    row_index = lax.broadcasted_iota(jnp.int32, (rows, width), 0)
    first_row, last_row = row_index == 0, row_index == last

    def shift_y(tile):
        return pltpu.roll(tile, 1, 1)

    def next_y(tile):
        return pltpu.roll(tile, width - 1, 1)

    def plane_move(j, b, v):
        return remote(
            v.at[0, b], plane_in.at[j, b], halo_send.at[j, b, 0], halo_recv.at[j, b, 0], (prv, k)
        )

    def part_move(j, b):
        return remote(
            plane_out.at[j, b], part_in.at[j, b], halo_send.at[j, b, 1], halo_recv.at[j, b, 1], (nxt, k)
        )

    def row_moves(j):
        return [
            remote(row_out.at[j], row_in.at[j], row_send.at[j, 0], row_recv.at[j, 0], (e, down)),
            remote(rowpart_out.at[j], rowpart_in.at[j], row_send.at[j, 1], row_recv.at[j, 1], (e, up)),
        ]

    def looped(body):
        def step(i, carry):
            body(i)
            return carry

        lax.fori_loop(0, 4, step, 0)

    def start_rows(j, v):
        def edge(a):
            for c in range(4):
                row_out[j, a, pl.ds(c, 1), :] = v[a, 0, c, pl.ds(0, 1), :]
                rowpart_out[j, a, pl.ds(c, 1), :] = c1[a, c, pl.ds(last, 1), :] * combine(
                    4, [v[a, b, c, pl.ds(last, 1), :] for b in range(4)]
                )

        looped(edge)
        for move in row_moves(j):
            move.start()

    def local_part(v, out, between=None):
        def along_x(b):
            for c in range(4):
                tiles = [v[a, b, c] for a in range(4)]
                scale = c0[b, c]
                out[0, b, c] = scale * combine(0, tiles) + c0p[b, c] * tiles[0]
                for a in range(1, 4):
                    out[a, b, c] = scale * combine(a, tiles)

        looped(along_x)

        def along_y(a):
            for b in range(4):
                tiles = [v[a, b, c] for c in range(4)]
                scale = c2[a, b]
                above = next_y(tiles[0])
                carried = shift_y(scale * combine(4, tiles))
                for c in range(4):
                    value = scale * (combine(c, tiles) + above * STIFF[c][4])
                    if c == 0:
                        value = value + carried + c2s[a, b] * tiles[0]
                    out[a, b, c] += value

        looped(along_y)
        if between is not None:
            between()

        def along_r(a):
            for c in range(4):
                tiles = [v[a, b, c] for b in range(4)]
                scale = c1[a, c]
                above = jnp.where(last_row, 0.0, pltpu.roll(tiles[0], rows - 1, 0))
                carried = jnp.where(first_row, 0.0, pltpu.roll(scale * combine(4, tiles), 1, 0))
                for b in range(4):
                    value = scale * (combine(b, tiles) + above * STIFF[b][4])
                    if b == 0:
                        value = value + carried + c1s[a, c] * tiles[0]
                    out[a, b, c] += value

        looped(along_r)

    def finish_rows(j, out):
        for move in row_moves(j):
            move.wait()

        def edge(a):
            for c in range(4):
                above = (has_above * row_in[j, a, pl.ds(c, 1), :]) * c1[a, c, pl.ds(last, 1), :]
                for b in range(4):
                    out[a, b, c, pl.ds(last, 1), :] += above * STIFF[b][4]
                out[a, 0, c, pl.ds(0, 1), :] += has_below * rowpart_in[j, a, pl.ds(c, 1), :]

        looped(edge)

    def streamed(j, v, out, update, following=None, sums=False):
        def quarter(b, carry):
            plane_move(j, b, v).wait()
            part_move(j, b).wait()
            for c in range(4):
                above = c0[b, c] * plane_in[j, b, c]
                tiles = []
                for a in range(4):
                    applied = out[a, b, c] + above * STIFF[a][4]
                    if a == 0:
                        applied = applied + part_in[j, b, c]
                    tile, terms = update(a, b, c, applied)
                    tiles.append(tile)
                    if sums:
                        carry = (carry[0] + terms[0], carry[1] + terms[1])
                if following is not None:
                    plane_out[j + 1, b, c] = c0[b, c] * combine(4, tiles)
            if following is not None:
                part_move(j + 1, b).start()
                plane_move(j + 1, b, following).start()
            return carry

        zero = jnp.zeros((rows, width), F32)
        return lax.fori_loop(0, 4, quarter, (zero, zero) if sums else 0)

    looped(lambda b: plane_move(0, b, x).start())
    metric_moves[1].wait()

    def lower(tile, tile_below):
        edge_row = has_below * tile_below[last:, :]
        return jnp.where(first_row, edge_row, pltpu.roll(tile, 1, 0))

    def four(plain, other, along):
        both = plain + other
        return {
            (0, 0): plain, (1, 0): both,
            (0, 1): plain + along(plain), (1, 1): both + along(both),
        }

    def pick(table, first, second):
        scale = W[first] * W[second]
        return table[(int(first == 0), int(second == 0))] * scale

    table_0 = four(own[0], lower(own[0], below[0]), shift_y)
    for i in range(4):
        for j in range(4):
            c0[i, j] = pick(table_0, i, j)

    def first_planes(b):
        for c in range(4):
            plane_out[0, b, c] = c0[b, c] * combine(4, [x[a, b, c] for a in range(4)])
        part_move(0, b).start()

    looped(first_planes)
    metric_moves[0].wait()
    metric_moves[2].wait()
    own_1, own_2 = own[1], own[2]
    prev_0, prev_1, prev_2 = prev[0], prev[1], prev[2]
    below_1, below_2 = below[1], below[2]
    diag_0, diag_1, diag_2 = diag[0], diag[1], diag[2]
    table_0p = four(prev_0, lower(prev_0, diag_0), shift_y)
    table_1 = four(own_1, prev_1, shift_y)
    table_1b = four(below_1, diag_1, shift_y)
    lower_2, lower_2p = lower(own_2, below_2), lower(prev_2, diag_2)
    table_2 = {
        (0, 0): own_2, (0, 1): own_2 + lower_2,
        (1, 0): own_2 + prev_2, (1, 1): own_2 + lower_2 + prev_2 + lower_2p,
    }
    for i in range(4):
        for j in range(4):
            c0p[i, j] = pick(table_0p, i, j) * STIFF[4][4]
            line = pick(table_1, i, j)
            c1[i, j] = line
            c1s[i, j] = lower(line, pick(table_1b, i, j)) * STIFF[4][4]
            line = pick(table_2, i, j)
            c2[i, j] = line
            c2s[i, j] = shift_y(line) * STIFF[4][4]

    start_rows(0, x)
    loads[2].wait()
    to_blocks(source_in, r)

    def diagonal(a):
        for b in range(4):
            for c in range(4):
                zero_a = jnp.where(a == 0, 1.0, 0.0).astype(F32)
                middle = jnp.where(a == 2, STIFF[2][2], STIFF[1][1]).astype(F32)
                stiff = jnp.where(a == 0, STIFF[0][0], middle).astype(F32)
                total = c0[b, c] * stiff + c0p[b, c] * zero_a
                total = total + c1[a, c] * STIFF[b][b]
                total = total + c2[a, b] * STIFF[c][c]
                if b == 0:
                    total = total + c1s[a, c]
                if c == 0:
                    total = total + c2s[a, b]
                inv[a, b, c] = 1.0 / total

    looped(diagonal)
    def rad_moves(t):
        return [
            remote(rad_out.at[t], rad_in.at[t, d - 1], rad_send.at[t, d - 1],
                   rad_recv.at[t, d - 1], (e, lax.rem(k + d, n_rad)))
            for d in range(1, n_rad)
        ]

    def group_moves(t):
        return [
            remote(group_out.at[t], group_in.at[t, d - 1], group_send.at[t, d - 1],
                   group_recv.at[t, d - 1], (lax.rem(e + d, n_group), k))
            for d in range(1, n_group)
        ]

    def lane_sum(tile):
        row = jnp.sum(tile, axis=0, keepdims=True)
        total = row[:, :128]
        for h in range(1, width // 128):
            total = total + row[:, h * 128:(h + 1) * 128]
        return total

    def sums_begin(t, gamma_tile, delta_tile):
        index = lax.broadcasted_iota(jnp.int32, (8, 128), 0)
        rad_out[t] = jnp.where(
            index == 0, lane_sum(gamma_tile), jnp.where(index == 1, lane_sum(delta_tile), 0.0)
        )
        for move in rad_moves(t):
            move.start()

    def sums_middle(t):
        total = rad_out[t]
        for d, move in enumerate(rad_moves(t)):
            move.wait()
            total = total + rad_in[t, d]
        group_out[t] = total
        for move in group_moves(t):
            move.start()

    def sums_end(t):
        total = group_out[t]
        for d, move in enumerate(group_moves(t)):
            move.wait()
            total = total + group_in[t, d]
        total = jnp.sum(total, axis=1, keepdims=True)
        return total[0:1, :], total[1:2, :]

    local_part(x, n)
    finish_rows(0, n)

    def initial(a, b, c, applied):
        residual = r[a, b, c] - applied
        r[a, b, c] = residual
        smooth = inv[a, b, c] * residual
        u[a, b, c] = smooth
        return smooth, None

    streamed(0, x, n, initial, u)
    start_rows(1, u)
    local_part(u, w)
    finish_rows(1, w)

    def first_sums(a, b, c, applied):
        w[a, b, c] = applied
        value = u[a, b, c]
        smooth = inv[a, b, c] * applied
        m_first[a, b, c] = smooth
        return smooth, (r[a, b, c] * value, applied * value)

    tiles = streamed(1, u, w, first_sums, m_first, True)
    sums_begin(0, *tiles)
    start_rows(2, m_first)
    local_part(m_first, z, lambda: sums_middle(0))
    finish_rows(2, z)
    gamma_0, delta_0 = sums_end(0)
    alpha_0 = gamma_0 / delta_0
    step = jnp.broadcast_to(alpha_0, (rows, width))

    def first_update(a, b, c, powered):
        z[a, b, c] = powered
        applied, search = w[a, b, c], u[a, b, c]
        s[a, b, c] = applied
        p[a, b, c] = search
        x[a, b, c] += step * search
        residual = r[a, b, c] - step * applied
        r[a, b, c] = residual
        scale = inv[a, b, c]
        smooth = scale * residual
        u[a, b, c] = smooth
        applied = applied - step * powered
        w[a, b, c] = applied
        powered = scale * applied
        m_second[a, b, c] = powered
        return powered, (residual * smooth, applied * smooth)

    tiles = streamed(2, m_first, z, first_update, m_second, True)
    sums_begin(1, *tiles)
    start_rows(3, m_second)
    local_part(m_second, n, lambda: sums_middle(1))
    finish_rows(3, n)
    gamma_1, delta_1 = sums_end(1)
    beta_0 = gamma_1 / gamma_0
    alpha_1 = gamma_1 / (delta_1 - beta_0 * gamma_1 / alpha_0)
    step_1 = jnp.broadcast_to(alpha_1, (rows, width))
    ratio_1 = jnp.broadcast_to(beta_0, (rows, width))

    def second_update(a, b, c, powered):
        applied = w[a, b, c]
        searched = applied + ratio_1 * s[a, b, c]
        s[a, b, c] = searched
        search = u[a, b, c] + ratio_1 * p[a, b, c]
        p[a, b, c] = search
        x[a, b, c] += step_1 * search
        residual = r[a, b, c] - step_1 * searched
        r[a, b, c] = residual
        smooth = inv[a, b, c] * residual
        u[a, b, c] = smooth
        applied = applied - step_1 * (powered + ratio_1 * z[a, b, c])
        w[a, b, c] = applied
        return applied, (residual * smooth, applied * smooth)

    tiles = streamed(3, m_second, n, second_update, None, True)
    sums_begin(2, *tiles)
    sums_middle(2)
    lane_join = one_where(i1 == 4 * (i0 % part) + i0 // part)
    row_join = one_where(r0 == split_row(r1))
    gamma_2, delta_2 = sums_end(2)
    beta_1 = gamma_2 / gamma_1
    alpha_2 = gamma_2 / (delta_2 - beta_1 * gamma_2 / alpha_1)
    step_2 = jnp.broadcast_to(alpha_2, (rows, width))
    ratio_2 = jnp.broadcast_to(beta_1, (rows, width))

    def last_update(a):
        for b in range(4):
            for c in range(4):
                x[a, b, c] += step_2 * (u[a, b, c] + ratio_2 * p[a, b, c])
                r[a, b, c] -= step_2 * (w[a, b, c] + ratio_2 * s[a, b, c])

    looped(last_update)

    def from_blocks(field, target):
        for h in range(lanes // CHUNK):
            wide = jnp.concatenate(
                [field[:, :, c, :, h * part:(h + 1) * part] for c in range(4)], axis=-1
            ).reshape(nodes, CHUNK)
            total = None
            for piece in exact_pieces(wide)[:2]:
                moved = dot(piece, lane_join).astype(BF16)
                moved = dot(row_join, moved)
                total = moved if total is None else total + moved
            target[:, :, h * CHUNK:(h + 1) * CHUNK] = total.reshape(4, block, CHUNK)

    from_blocks(x, guess_in)
    store_x = pltpu.make_async_copy(guess_in, sol_hbm, local_sem.at[3])
    store_x.start()
    from_blocks(r, source_in)
    store_r = pltpu.make_async_copy(source_in, res_hbm, local_sem.at[4])
    store_r.start()
    store_x.wait()
    store_r.wait()


def solution(mesh):
    n_group, n_rad = mesh.shape["group"], mesh.shape["rad"]

    def local(source_term, initial_guess, metric):
        shape = source_term.shape
        metric = metric.reshape(3, metric.shape[2], metric.shape[3])
        rows, width = metric.shape[1:]
        assert shape == (4, 4 * rows, 4 * width) and rows % 8 == 0 and shape[2] % CHUNK == 0
        tile = (rows, width)
        field = pltpu.VMEM((4, 4, 4) + tile, F32)
        plane = pltpu.VMEM((4, 4) + tile, F32)
        planes = pltpu.VMEM((APPLIES, 4, 4) + tile, F32)
        edges = pltpu.VMEM((APPLIES, 4, 4, width), F32)
        any_space = pl.BlockSpec(memory_space=pl.ANY)
        return pl.pallas_call(
            functools.partial(kernel, n_group, n_rad),
            out_shape=[jax.ShapeDtypeStruct(shape, F32)] * 2,
            in_specs=[any_space] * 3,
            out_specs=[any_space] * 2,
            scratch_shapes=[
                pltpu.VMEM(shape, F32), pltpu.VMEM(shape, F32),
                *[pltpu.VMEM((3,) + tile, F32)] * 4,
                *[plane] * 6, field,
                *[field] * 10,
                planes, planes, planes, edges, edges, edges, edges,
                pltpu.VMEM((ITERS, 8, 128), F32), pltpu.VMEM((ITERS, n_rad - 1, 8, 128), F32),
                pltpu.VMEM((ITERS, 8, 128), F32), pltpu.VMEM((ITERS, n_group - 1, 8, 128), F32),
                pltpu.SemaphoreType.DMA((5,)),
                pltpu.SemaphoreType.DMA((3,)), pltpu.SemaphoreType.DMA((3,)),
                pltpu.SemaphoreType.DMA((APPLIES, 4, 2)), pltpu.SemaphoreType.DMA((APPLIES, 4, 2)),
                pltpu.SemaphoreType.DMA((APPLIES, 2)), pltpu.SemaphoreType.DMA((APPLIES, 2)),
                pltpu.SemaphoreType.DMA((ITERS, n_rad - 1)), pltpu.SemaphoreType.DMA((ITERS, n_rad - 1)),
                pltpu.SemaphoreType.DMA((ITERS, n_group - 1)), pltpu.SemaphoreType.DMA((ITERS, n_group - 1)),
            ],
            compiler_params=pltpu.CompilerParams(
                collective_id=0, has_side_effects=True, vmem_limit_bytes=63 * 1024 * 1024
            ),
            name="pcg",
        )(source_term, initial_guess, metric)

    in_specs = (P("group", "rad", None), P("group", "rad", None), P(None, "group", "rad", None))
    out_specs = (P("group", "rad", None), P("group", "rad", None))
    return jax.shard_map(local, mesh=mesh, in_specs=in_specs, out_specs=out_specs, check_vma=False)
```
